32 devices in a mesh: grp: 4 (over y, core), seq: 8 (over z, x).
Axes of the slice: x: 2, y: 2, z: 4, core: 2. Of those that a mesh axis runs over, the one named last changes fastest.
Arguments:
- layer_input: bfloat16 [8192, 2048], P(('grp', 'seq')), may hold values from -6 to 6
- entry_gain: float32 [2048], replicated, may hold values from 0.1 to 1.9
- entry_shift: float32 [2048], replicated, may hold values from -1.75 to 1.75
- joint_weight: bfloat16 [2048, 6144], P(('grp', 'seq')), may hold values from -0.125 to 0.125
- query_offset: float32 [2048], replicated, may hold values from -3 to 3
- value_offset: float32 [2048], replicated, may hold values from -0.3125 to 0.3125
- mixing_weight: bfloat16 [2048, 2048], P(('grp', 'seq')), may hold values from -1 to 1
- attention_offset: float32 [2048], replicated, may hold values from -3 to 3
- middle_gain: float32 [2048], replicated, may hold values from 0.1 to 1.9
- middle_shift: float32 [2048], replicated, may hold values from -1.75 to 1.75
- expand_weight: bfloat16 [2048, 8192], P(('grp', 'seq')), may hold values from -0.125 to 0.125
- expand_offset: float32 [8192], replicated, may hold values from -3 to 3
- shrink_weight: bfloat16 [2048, 8192], P(('grp', 'seq')), may hold values from -0.0625 to 0.0625
- shrink_offset: float32 [2048], replicated, may hold values from -3 to 3
- placement: int32 [4, 2048], P('grp'), may hold values from 0 to 2047, each once within a row
- slot_lengths: int32 [4, 4], P('grp'), may hold values from 1 to 256, 832 in all within a row
- cotangent: bfloat16 [8192, 2048], P(('grp', 'seq')), may hold values from -6 to 6
Outputs:
- layer_output: bfloat16 [8192, 2048], P(('grp', 'seq'))
- input_gradient: bfloat16 [8192, 2048], P(('grp', 'seq'))
- entry_gain_gradient: float32 [2048], replicated
- entry_shift_gradient: float32 [2048], replicated
- joint_gradient: float32 [2048, 6144], P(('grp', 'seq'))
- query_gradient: float32 [2048], replicated
- value_gradient: float32 [2048], replicated
- mixing_gradient: float32 [2048, 2048], P(('grp', 'seq'))
- attention_offset_gradient: float32 [2048], replicated
- middle_gain_gradient: float32 [2048], replicated
- middle_shift_gradient: float32 [2048], replicated
- expand_gradient: float32 [2048, 8192], P(('grp', 'seq'))
- expand_offset_gradient: float32 [8192], replicated
- shrink_gradient: float32 [2048, 8192], P(('grp', 'seq'))
- shrink_offset_gradient: float32 [2048], replicated
The draws below stay inside these ranges and needn't reach their ends.
Inputs may be any that keep to these rules, and one draw needn't show every extreme that they name: `placement`: each row holds every position of its group once. `slot_lengths`: the real tokens of each slot of 256 positions; the rest of a slot is padding; some slot of every group is full.
All inputs are finite; a program needn't handle non-finite values.
Results may differ from the reference program's by a relative error of at most 0.013.
Values may be sent and summed in bfloat16 or wider, within the bound.
A program may use at most 704 MiB of HBM per device.

```python
import math
import jax
import jax.numpy as jnp
import numpy as np
from jax import lax

D = 2048
HEADS = 16
HEAD = 128
FF = 8192
CONT = 256
QBLOCK = 512
GROUPS = 4
GROUP_TOK = 2048
PROMPT = 1024
NCONT = 4
TOKENS = 8192


def level_of(stream_key, extent, cuts, smallest, top_value):
    factor_of, own = 1.0, jax.random.fold_in(stream_key, 6)
    for dim, shards_of in cuts:
        draws = jnp.exp(jax.random.uniform(jax.random.fold_in(own, dim), (shards_of,), jnp.float32, smallest / len(cuts), top_value / len(cuts)))
        factor_of = factor_of * jnp.repeat(draws, extent[dim] // shards_of).reshape([-1 if axis == dim else 1 for axis in range(len(extent))])
    return factor_of


def length_profile(number_of, total, most, lean):
    weights = [(1 << 20) // math.isqrt(grade ** lean) + 1 for grade in range(2, number_of + 1)]
    surplus, holding = total - most - (number_of - 1), [1] * (number_of - 1)
    while surplus > 0:
        candidates = [i for i in range(number_of - 1) if holding[i] < most]
        mass, left = sum([weights[i] for i in candidates]), surplus
        for i in candidates:
            extra = min(most - holding[i], max(1, left * weights[i] // mass), surplus)
            holding[i] = holding[i] + extra
            surplus = surplus - extra
    return np.array([most] + holding)


def ragged(rng, count, total, bound, lean):
    if count == 2:
        one = jax.random.randint(rng, (), max(1, total - bound), min(bound, total - 1) + 1)
        return jnp.stack([one, total - one])
    sizes = jnp.asarray(length_profile(count, total, bound, lean), jnp.int32)
    couples = (count - 1) // 2
    source_of, sink = sizes[1:1 + 2 * couples:2], sizes[2:2 + 2 * couples:2]
    slack = jnp.minimum(source_of - 1, bound - sink)
    passed = jax.random.randint(jax.random.fold_in(rng, 1), (couples,), 0, 1 << 20) % (slack + 1)
    sizes = sizes.at[1:1 + 2 * couples:2].set(source_of - passed).at[2:2 + 2 * couples:2].set(sink + passed)
    return sizes[jax.random.permutation(jax.random.fold_in(rng, 2), count)]


def normal_values(stream_key, dims, scale, reach, split=(), kind=jnp.bfloat16):
    level = level_of(stream_key, dims, split, -0.22, 0.18) if split else 1.0
    values = jax.random.normal(stream_key, dims, jnp.float32) * scale * level
    return jnp.minimum(jnp.maximum(values, -reach), reach).astype(kind)


def setup_inputs(seed: int = 0) -> dict:
    keys = jax.random.split(jax.random.key(seed), 18)
    layer_input = normal_values(keys[0], (TOKENS, D), 1.0, 6.0, ((0, 32),))
    entry_gain = jnp.clip(1.0 + 0.18 * jax.random.normal(keys[1], (D,), jnp.float32), 0.1, 1.9)
    entry_shift = normal_values(keys[2], (D,), 0.3, 1.75, (), jnp.float32)
    joint_weight = normal_values(keys[3], (D, 3 * D), D ** -0.5, 0.125, ((0, 32),))
    query_offset = normal_values(keys[4], (D,), 0.5, 3.0, (), jnp.float32)
    value_offset = normal_values(keys[5], (D,), 0.05, 0.3125, (), jnp.float32)
    mixing_weight = normal_values(keys[6], (D, D), (D // 64) ** -0.5, 1.0, ((0, 32),))
    attention_offset = normal_values(keys[7], (D,), 0.5, 3.0, (), jnp.float32)
    middle_gain = jnp.clip(1.0 + 0.18 * jax.random.normal(keys[8], (D,), jnp.float32), 0.1, 1.9)
    middle_shift = normal_values(keys[9], (D,), 0.3, 1.75, (), jnp.float32)
    expand_weight = normal_values(keys[10], (D, FF), D ** -0.5, 0.125, ((0, 32),))
    expand_offset = normal_values(keys[11], (FF,), 0.5, 3.0, (), jnp.float32)
    shrink_weight = normal_values(keys[12], (D, FF), FF ** -0.5, 0.0625, ((0, 32),))
    shrink_offset = normal_values(keys[13], (D,), 0.5, 3.0, (), jnp.float32)
    placement = jax.vmap(lambda own: jax.random.permutation(own, GROUP_TOK))(jax.random.split(keys[14], GROUPS)).reshape((GROUPS, GROUP_TOK)).astype(jnp.int32)
    slot_lengths = jax.vmap(lambda own: ragged(own, NCONT, (3 * NCONT + 1) * CONT // 4, CONT, 2))(jax.random.split(keys[15], GROUPS)).reshape((GROUPS, NCONT)).astype(jnp.int32)
    cotangent = normal_values(keys[16], (TOKENS, D), 1.0, 6.0, ((0, 32),))
    return dict(layer_input=layer_input, entry_gain=entry_gain, entry_shift=entry_shift, joint_weight=joint_weight, query_offset=query_offset, value_offset=value_offset, mixing_weight=mixing_weight, attention_offset=attention_offset, middle_gain=middle_gain, middle_shift=middle_shift, expand_weight=expand_weight, expand_offset=expand_offset, shrink_weight=shrink_weight, shrink_offset=shrink_offset, placement=placement, slot_lengths=slot_lengths, cotangent=cotangent)


@jax.custom_vjp
def low(v):
    return lax.optimization_barrier(v.astype(jnp.bfloat16)).astype(jnp.float32)

@jax.custom_vjp
def low_back(v):
    return v

def low_keep(v):
    return (low(v), None)

def low_pass(kept, grad):
    return (grad,)

def back_keep(v):
    return (v, None)

def back_low(kept, grad):
    return (low(grad),)
low.defvjp(low_keep, low_pass)
low_back.defvjp(back_keep, back_low)
highest = lax.Precision.HIGHEST
norm_epsilon = 1e-05
masked_score = -1e+30

def product(left_matrix, right_matrix):
    return jnp.dot(left_matrix, right_matrix, precision=highest, preferred_element_type=jnp.float32)

def layer_norm(values, scale_vector, shift_vector):
    average = lax.optimization_barrier(jnp.mean(values, axis=-1, keepdims=True))
    centered = values - average
    variance = lax.optimization_barrier(jnp.mean(centered * centered, axis=-1, keepdims=True))
    return centered * lax.rsqrt(variance + norm_epsilon) * scale_vector + shift_vector

def key_facts(positions, lengths):
    segment = (positions - PROMPT) // CONT
    within = positions - PROMPT - segment * CONT
    slot_ids = jnp.arange(lengths.shape[0], dtype=jnp.int32)
    slot_limit = lax.optimization_barrier(jnp.sum(jnp.where(segment[:, None] == slot_ids[None, :], lengths[None, :], 0), axis=1))
    return (segment, (positions < PROMPT) | (within < slot_limit))

def block_mask(query_place, key_place, key_segment, key_live):
    query_col = query_place[:, None]
    key_row = key_place[None, :]
    query_segment = (query_col - PROMPT) // CONT
    prompt_keys = (key_row < PROMPT) & ((query_col >= PROMPT) | (key_row <= query_col))
    same_slot = (query_col >= PROMPT) & (key_row >= PROMPT) & (query_segment == key_segment[None, :]) & (key_row <= query_col) & key_live[None, :]
    return prompt_keys | same_slot

def group_forward(param_tuple, tokens, positions, lengths):
    entry_gain, entry_shift, joint_weight, query_offset, value_offset, mixing_weight, attention_offset, middle_gain, middle_shift, expand_weight, expand_offset, shrink_weight, shrink_offset = param_tuple
    entry_normed = low(layer_norm(tokens, entry_gain, entry_shift))
    offsets = jnp.stack([query_offset.reshape(HEADS, HEAD), jnp.zeros((HEADS, HEAD), jnp.float32), value_offset.reshape(HEADS, HEAD)], axis=1)
    joint_values = product(entry_normed, joint_weight).reshape(GROUP_TOK, HEADS, 3, HEAD) + offsets
    joint_values = low(low_back(joint_values))
    queries = joint_values[:, :, 0]
    key_vectors = joint_values[:, :, 1]
    values = joint_values[:, :, 2]
    key_segment, key_live = key_facts(positions, lengths)
    score_scale = HEAD ** (-0.5)

    def one_block(block_args):
        block_queries, block_places = block_args
        scores = jnp.einsum('qhe,khe->hqk', block_queries, key_vectors, precision=highest) * score_scale
        allowed = block_mask(block_places, positions, key_segment, key_live)
        scores = low_back(jnp.where(allowed[None], scores, masked_score))
        soft_weights = low(jax.nn.softmax(scores, axis=-1))
        return jnp.einsum('hqk,khe->qhe', soft_weights, values, precision=highest)
    blocks = GROUP_TOK // QBLOCK
    mixture = lax.map(jax.checkpoint(one_block), (queries.reshape(blocks, QBLOCK, HEADS, HEAD), positions.reshape(blocks, QBLOCK)))
    attended = low(low_back(mixture.reshape(GROUP_TOK, D)))
    branch = low_back(product(attended, mixing_weight) + attention_offset)
    residual = tokens + branch
    middle_normed = low(layer_norm(residual, middle_gain, middle_shift))
    expanded = low_back(product(middle_normed, expand_weight) + expand_offset)
    activated = low(jax.nn.gelu(expanded, approximate=False))
    return residual + product(activated, shrink_weight.T) + shrink_offset

def reference(layer_input, entry_gain, entry_shift, joint_weight, query_offset, value_offset, mixing_weight, attention_offset, middle_gain, middle_shift, expand_weight, expand_offset, shrink_weight, shrink_offset, placement, slot_lengths, cotangent):
    param_tuple = (entry_gain, entry_shift, joint_weight.astype(jnp.float32), query_offset, value_offset, mixing_weight.astype(jnp.float32), attention_offset, middle_gain, middle_shift, expand_weight.astype(jnp.float32), expand_offset, shrink_weight.astype(jnp.float32), shrink_offset)
    tokens_float = layer_input.astype(jnp.float32).reshape(GROUPS, GROUP_TOK, D)

    def whole(tokens_all, params_all):

        def scan_step(running, group_args):
            tokens, positions, lengths = group_args
            return (running, group_forward(params_all, tokens, positions, lengths))
        unused_total, outputs = lax.scan(scan_step, jnp.zeros((), jnp.float32), (tokens_all, placement, slot_lengths))
        return outputs
    output_float, pullback = jax.vjp(whole, tokens_float, param_tuple)
    input_slope, slopes = pullback(cotangent.astype(jnp.float32).reshape(GROUPS, GROUP_TOK, D))
    return (output_float.reshape(TOKENS, D).astype(jnp.bfloat16), input_slope.reshape(TOKENS, D).astype(jnp.bfloat16), slopes[0], slopes[1], slopes[2], slopes[3], slopes[4], slopes[5], slopes[6], slopes[7], slopes[8], slopes[9], slopes[10], slopes[11], slopes[12])
```

```python
import functools

import jax
import jax.numpy as jnp
from jax import lax
from jax.experimental import pallas as pl
from jax.experimental.pallas import tpu as pltpu
from jax.sharding import Mesh
from jax.sharding import PartitionSpec as P

HEADS = 16
CONT = 256
ALL = ("y", "c", "z", "x")
norm_epsilon = 1e-05
masked_score = -1e30
f32 = jnp.float32
bf16 = jnp.bfloat16


def dot_f32(a, b, dims):
    return lax.dot_general(a, b, (dims, ((), ())), preferred_element_type=f32)


def dot_nn(a, b):
    return dot_f32(a, b, ((1,), (0,)))


def dot_nt(a, b):
    return dot_f32(a, b, ((1,), (1,)))


def dot_tn(a, b):
    return dot_f32(a, b, ((0,), (0,)))


def forward_kernel(hl, scale2, j_ref, qa_ref, qlo_ref, ka_ref, kb_ref, o_ref, lt_ref, vt_ref):
    step = pl.program_id(0)
    block = o_ref.shape[0]
    head = o_ref.shape[1] // hl

    @pl.when(step == 0)
    def _():
        for h in range(hl):
            base = 3 * h * head
            vt_ref[h] = jnp.transpose(j_ref[:, base + 2 * head : base + 3 * head])

    rows = pl.ds(pl.multiple_of(step * block, block), block)
    allowed = (ka_ref[...] <= qa_ref[...]) & (kb_ref[...] >= qlo_ref[...])
    for h in range(hl):
        base = 3 * h * head
        queries = j_ref[rows, base : base + head]
        keys = j_ref[:, base + head : base + 2 * head]
        scores = jnp.where(allowed, dot_nt(keys, queries) * scale2, masked_score)
        top = jnp.max(scores, axis=0, keepdims=True)
        weights = jnp.exp2(scores - top)
        total = jnp.sum(weights, axis=0, keepdims=True)
        mixed = dot_nn(vt_ref[h], weights.astype(bf16)) / total
        o_ref[:, h * head : (h + 1) * head] = jnp.transpose(mixed).astype(bf16)
        lt_ref[0, h : h + 1, :] = top + jnp.log2(total)


def backward_kernel(
    hl, scale, scale2, j_ref, do_ref, lt_ref, qa_ref, qlo_ref, ka_ref, kb_ref, dj_ref, kt_ref, dk_ref, dv_ref
):
    step = pl.program_id(0)
    block = do_ref.shape[0]
    head = do_ref.shape[1] // hl

    @pl.when(step == 0)
    def _():
        for h in range(hl):
            base = 3 * h * head
            kt_ref[h] = jnp.transpose(j_ref[:, base + head : base + 2 * head])
        dk_ref[...] = jnp.zeros_like(dk_ref)
        dv_ref[...] = jnp.zeros_like(dv_ref)

    rows = pl.ds(pl.multiple_of(step * block, block), block)
    allowed = (ka_ref[...] <= qa_ref[...]) & (kb_ref[...] >= qlo_ref[...])
    for h in range(hl):
        base = 3 * h * head
        queries = j_ref[rows, base : base + head]
        keys = j_ref[:, base + head : base + 2 * head]
        values = j_ref[:, base + 2 * head : base + 3 * head]
        slopes = do_ref[:, h * head : (h + 1) * head]
        scores = jnp.where(allowed, dot_nt(keys, queries) * scale2, masked_score)
        probable = jnp.exp2(scores - lt_ref[0, h : h + 1, :])
        weight_slope = dot_nt(values, slopes)
        centre = jnp.sum(probable * weight_slope, axis=0, keepdims=True)
        score_slope = (probable * (weight_slope - centre)).astype(bf16)
        dv_ref[h] += dot_nn(probable.astype(bf16), slopes)
        dk_ref[h] += dot_nn(score_slope, queries)
        query_slope = dot_nn(kt_ref[h], score_slope) * scale
        dj_ref[rows, base : base + head] = jnp.transpose(query_slope).astype(bf16)

    @pl.when(step == pl.num_programs(0) - 1)
    def _():
        for h in range(hl):
            base = 3 * h * head
            dj_ref[:, base + head : base + 2 * head] = (dk_ref[h] * scale).astype(bf16)
            dj_ref[:, base + 2 * head : base + 3 * head] = dv_ref[h].astype(bf16)


def whole(shape):
    return pl.BlockSpec(shape, lambda i: (0,) * len(shape), pipeline_mode=pl.Buffered(1))


def attention_block(rows):
    return 256 if rows % 256 == 0 else 128


def attention_forward(joint, qa, qlo, ka, kb, hl, head):
    rows = joint.shape[0]
    block = attention_block(rows)
    steps = rows // block
    scale2 = head ** (-0.5) * 1.4426950408889634
    return pl.pallas_call(
        functools.partial(forward_kernel, hl, scale2),
        grid=(steps,),
        out_shape=(
            jax.ShapeDtypeStruct((rows, hl * head), bf16),
            jax.ShapeDtypeStruct((steps, hl, block), f32),
        ),
        in_specs=[
            whole(joint.shape),
            pl.BlockSpec((1, block), lambda i: (0, i)),
            pl.BlockSpec((1, block), lambda i: (0, i)),
            whole((rows, 1)),
            whole((rows, 1)),
        ],
        out_specs=(
            pl.BlockSpec((block, hl * head), lambda i: (i, 0)),
            pl.BlockSpec((1, hl, block), lambda i: (i, 0, 0)),
        ),
        scratch_shapes=[pltpu.VMEM((hl, head, rows), bf16)],
        cost_estimate=pl.CostEstimate(
            flops=4 * rows * rows * hl * head,
            bytes_accessed=rows * hl * head * 8,
            transcendentals=rows * rows * hl,
        ),
        name="attend",
    )(joint, qa, qlo, ka, kb)


def attention_backward(joint, slopes, totals, qa, qlo, ka, kb, hl, head):
    rows = joint.shape[0]
    block = attention_block(rows)
    steps = rows // block
    scale = head ** (-0.5)
    return pl.pallas_call(
        functools.partial(backward_kernel, hl, scale, scale * 1.4426950408889634),
        grid=(steps,),
        out_shape=jax.ShapeDtypeStruct(joint.shape, bf16),
        in_specs=[
            whole(joint.shape),
            pl.BlockSpec((block, hl * head), lambda i: (i, 0)),
            pl.BlockSpec((1, hl, block), lambda i: (i, 0, 0)),
            pl.BlockSpec((1, block), lambda i: (0, i)),
            pl.BlockSpec((1, block), lambda i: (0, i)),
            whole((rows, 1)),
            whole((rows, 1)),
        ],
        out_specs=whole(joint.shape),
        scratch_shapes=[
            pltpu.VMEM((hl, head, rows), bf16),
            pltpu.VMEM((hl, rows, head), f32),
            pltpu.VMEM((hl, rows, head), f32),
        ],
        cost_estimate=pl.CostEstimate(
            flops=10 * rows * rows * hl * head,
            bytes_accessed=rows * hl * head * 14,
            transcendentals=rows * rows * hl,
        ),
        name="attend_back",
    )(joint, slopes, totals, qa, qlo, ka, kb)


def pick(index, cases):
    return cases[0] if len(cases) == 1 else lax.select_n(index.astype(jnp.int32), *cases)


def norm_parts(values):
    average = jnp.mean(values, axis=-1, keepdims=True)
    centered = values - average
    variance = jnp.mean(centered * centered, axis=-1, keepdims=True)
    inverse = lax.rsqrt(variance + norm_epsilon)
    return centered * inverse, inverse


def norm_back(slope, gain, normal, inverse):
    scaled = slope * gain
    first = jnp.mean(scaled, axis=-1, keepdims=True)
    second = jnp.mean(scaled * normal, axis=-1, keepdims=True)
    return inverse * (scaled - first - normal * second)


def solution(mesh):
    groups, seqs = mesh.shape["grp"], mesh.shape["seq"]
    nc = 2 if groups % 2 == 0 else 1
    ny = groups // nc
    n1 = 4 if seqs % 4 == 0 else seqs
    n2 = seqs // n1
    sizes = (ny, nc, n1, n2)
    fine = Mesh(mesh.devices.reshape(sizes), ALL)
    plane = [(dy, dx) for dy in range(ny) for dx in range(n2)]

    def moves(target):
        pairs = []
        for y in range(ny):
            for c in range(nc):
                for z in range(n1):
                    for x in range(n2):
                        to = target(y, c, z, x)
                        if to is None:
                            continue
                        source = ((y * nc + c) * n1 + z) * n2 + x
                        dest = ((to[0] * nc + to[1]) * n1 + to[2]) * n2 + to[3]
                        pairs.append((source, dest))
        return pairs

    def send(value, target):
        return lax.ppermute(value, ALL, moves(target))

    def shift_plane(value, dy, dx):
        if dy % ny == 0 and dx % n2 == 0:
            return value
        return send(value, lambda y, c, z, x: ((y + dy) % ny, c, z, (x + dx) % n2))

    def shift_x(value, dx):
        return send(value, lambda y, c, z, x: (y, c, z, (x + dx) % n2))

    def swap_c(value, dc):
        return send(value, lambda y, c, z, x: (y, (c + dc) % nc, z, x))

    def up(value):
        return send(value, lambda y, c, z, x: (y, c, z + 1, x) if z + 1 < n1 else None)

    def down(value):
        return send(value, lambda y, c, z, x: (y, c, z - 1, x) if z > 0 else None)

    def line_gather(value, zi):
        rows = value.shape[0]
        above, below = [value], [value]
        for _ in range(n1 - 1):
            above.append(up(above[-1]))
            below.append(down(below[-1]))
        row = above[:0:-1] + below
        joined = jnp.concatenate(row, axis=0)
        return lax.dynamic_slice_in_dim(joined, (n1 - 1 - zi) * rows, n1 * rows, 0)

    def line_sum(blocks, zi):
        def at(index):
            inside = (index >= 0) & (index < n1)
            part = lax.dynamic_index_in_dim(blocks, jnp.clip(index, 0, n1 - 1), 0, keepdims=False)
            return jnp.where(inside, part.astype(f32), 0.0)

        rising, falling = 0.0, 0.0
        for k in range(1, n1):
            rising = up((at(n1 - k + zi) + rising).astype(bf16)).astype(f32)
            falling = down((at(zi - n1 + k) + falling).astype(bf16)).astype(f32)
        return at(zi) + rising + falling

    def shards(
        layer_input,
        entry_gain,
        entry_shift,
        joint_weight,
        query_offset,
        value_offset,
        mixing_weight,
        attention_offset,
        middle_gain,
        middle_shift,
        expand_weight,
        expand_offset,
        shrink_weight,
        shrink_offset,
        placement,
        slot_lengths,
        cotangent,
    ):
        yi, ci, zi, xi = (lax.axis_index(a) for a in ALL)
        tokens, width = layer_input.shape
        hidden = expand_weight.shape[1]
        own_rows = joint_weight.shape[0]
        head = width // HEADS
        hl = HEADS // seqs
        span = hl * head
        np_ = ny * n2
        part = hidden // np_
        line = n1 * tokens
        plane_index = yi * n2 + xi

        input_float = layer_input.astype(f32)
        normal1, inverse1 = norm_parts(input_float)
        entry_normed = (normal1 * entry_gain + entry_shift).astype(bf16)
        line_normed = line_gather(entry_normed, zi)

        columns = 3 * width // n1
        mine = lax.all_to_all(
            jnp.transpose(joint_weight.reshape(own_rows, n1, columns), (1, 0, 2)), "z", 0, 0, tiled=True
        )
        joint_cols = lax.all_gather(mine, ("y", "c", "x"), axis=0, tiled=False)
        joint_cols = jnp.transpose(
            joint_cols.reshape(ny, nc, n2, n1, own_rows, columns), (0, 1, 3, 2, 4, 5)
        ).reshape(width, columns)

        def hidden_part(weight):
            blocks = jnp.transpose(weight.reshape(own_rows, np_, part), (1, 0, 2))
            blocks = lax.all_to_all(blocks, ("y", "x"), 0, 0, tiled=True)
            return lax.all_gather(
                blocks.reshape(np_ * own_rows, part), ("c", "z"), axis=0, tiled=True
            )

        def permuted(values):
            rows = values.shape[0]
            return jnp.transpose(
                values.reshape(rows, ny, nc, n1, n2 * own_rows), (0, 2, 3, 1, 4)
            ).reshape(rows, width)

        def natural(values):
            rows = values.shape[0]
            return jnp.transpose(
                values.reshape(rows, nc, n1, ny, n2 * own_rows), (0, 3, 1, 2, 4)
            ).reshape(rows, width)

        offsets = jnp.stack(
            [
                query_offset.reshape(HEADS, head),
                jnp.zeros((HEADS, head), f32),
                value_offset.reshape(HEADS, head),
            ],
            axis=1,
        ).reshape(n1, columns)
        joint_values = (
            dot_nn(line_normed, joint_cols)
            + lax.dynamic_index_in_dim(offsets, zi, 0, keepdims=True)
        ).astype(bf16)

        def columns_of(index):
            return lax.dynamic_slice_in_dim(joint_values, index * 3 * span, 3 * span, 1)

        kept = jnp.concatenate(
            [columns_of(xi)] + [shift_x(columns_of((xi + r) % n2), r) for r in range(1, n2)], axis=0
        )

        places = placement[0]
        prompt = places.shape[0] // 2
        segment = (places - prompt) // CONT
        within = places - prompt - segment * CONT
        limit = jnp.sum(
            jnp.where(
                segment[:, None] == jnp.arange(slot_lengths.shape[1], dtype=jnp.int32)[None, :],
                slot_lengths[0][None, :],
                0,
            ),
            axis=1,
        )
        far = jnp.int32(1 << 30)
        key_a = jnp.where((places < prompt) | (within < limit), places, far)
        key_b = jnp.where(places < prompt, far, places)
        query_low = jnp.where(places < prompt, 0, prompt + segment * CONT)

        def relative(vector):
            grid = jnp.transpose(vector.reshape(n1, n2, tokens), (1, 0, 2)).reshape(n2, line)
            return jnp.concatenate(
                [lax.dynamic_index_in_dim(grid, (xi - r) % n2, 0, keepdims=False) for r in range(n2)]
            )

        masks = (
            relative(places)[None, :],
            relative(query_low)[None, :],
            relative(key_a)[:, None],
            relative(key_b)[:, None],
        )
        mixture, log_totals = attention_forward(kept, *masks, hl, head)

        def reorder(values):
            cases = [values[r] for r in range(n2)]
            return jnp.stack([pick((xi - r) % n2, cases) for r in range(n2)])

        outgoing = reorder(mixture.reshape(n2, n1, tokens, span)).reshape(seqs, tokens, span)
        arrived = lax.all_to_all(outgoing, ("x", "z"), 0, 0, tiled=True)
        attended = jnp.transpose(arrived.reshape(n2, n1, tokens, span), (2, 1, 0, 3)).reshape(
            tokens, width
        )

        mixing_full = lax.all_gather(mixing_weight, ALL, axis=0, tiled=True)
        residual = input_float + (dot_nn(attended, mixing_full) + attention_offset)
        normal2, inverse2 = norm_parts(residual)
        middle_normed = permuted((normal2 * middle_gain + middle_shift).astype(bf16))

        shrink_part = hidden_part(shrink_weight)
        expand_part = hidden_part(expand_weight)
        own_offset = lax.dynamic_index_in_dim(
            expand_offset.reshape(np_, part), plane_index, 0, keepdims=True
        )
        cotangent_own = permuted(cotangent)
        cot_blocks = [shift_plane(cotangent_own, dy, dx) for dy, dx in plane]
        mid_blocks = [shift_plane(middle_normed, dy, dx) for dy, dx in plane]
        act_blocks, slope_blocks = [], []
        normed_back, output_back = [], []
        for (dy, dx), cot_block, mid_block in zip(plane, cot_blocks, mid_blocks):
            activated_slope = dot_nn(cot_block, shrink_part)
            expanded = dot_nn(mid_block, expand_part) + own_offset
            phi_sum = 0.5 + 0.5 * lax.erf(expanded * 0.7071067811865476)
            density = jnp.exp(-0.5 * expanded * expanded) * 0.3989422804014327
            activated = (expanded * phi_sum).astype(bf16)
            slope = (activated_slope * (phi_sum + expanded * density)).astype(bf16)
            act_blocks.append(activated)
            slope_blocks.append(slope)
            back_n = dot_nt(slope, expand_part)
            back_y = dot_nt(activated, shrink_part)
            if (dy, dx) != (0, 0):
                back_n = shift_plane(back_n.astype(bf16), -dy, -dx)
                back_y = shift_plane(back_y.astype(bf16), -dy, -dx)
            normed_back.append(back_n)
            output_back.append(back_y)

        def total(parts):
            result = parts[0]
            for other in parts[1:]:
                result = result + other.astype(f32)
            return result

        layer_output = (residual + natural(total(output_back)) + shrink_offset).astype(bf16)
        normed_slope = natural(total(normed_back))
        residual_slope = cotangent.astype(f32) + norm_back(
            normed_slope, middle_gain, normal2, inverse2
        )
        branch_slope = residual_slope.astype(bf16)

        attended_slope = dot_nt(branch_slope, mixing_full).astype(bf16)
        outgoing = jnp.transpose(
            attended_slope.reshape(tokens, n1, n2, span), (2, 1, 0, 3)
        ).reshape(seqs, tokens, span)
        arrived = lax.all_to_all(outgoing, ("x", "z"), 0, 0, tiled=True)
        head_slopes = reorder(arrived.reshape(n2, line, span)).reshape(n2 * line, span)
        joint_heads = attention_backward(kept, head_slopes, log_totals, *masks, hl, head)
        own_sums = jnp.sum(joint_heads.astype(f32).reshape(n2 * line, hl, 3, head), axis=0)

        pieces = joint_heads.reshape(n2, line, 3 * span)
        gathered = [pieces[0]] + [shift_x(pieces[r], -r) for r in range(1, n2)]
        joint_slope = jnp.concatenate(
            [pick((r - xi) % n2, gathered) for r in range(n2)], axis=1
        )
        entry_partial = dot_nt(joint_slope, joint_cols).astype(bf16)
        entry_slope = line_sum(entry_partial.reshape(n1, tokens, width), zi)
        input_gradient = (
            residual_slope + norm_back(entry_slope, entry_gain, normal1, inverse1)
        ).astype(bf16)

        def chip_pair(left, right, last):
            halves = left.reshape(left.shape[0], nc, width // nc) if last else left
            own = 0.0
            for r in range(1, nc):
                other = lax.dynamic_index_in_dim(halves, (ci + r) % nc, 1, keepdims=False)
                own = own + swap_c(dot_tn(other, right).astype(bf16), r).astype(f32)
            here = lax.dynamic_index_in_dim(halves, ci, 1, keepdims=False)
            return dot_tn(here, right) + own

        def hidden_gradient(left, right):
            rows = chip_pair(left, right, True).astype(bf16)
            summed = line_sum(rows.reshape(n1, np_ * own_rows, part), zi).astype(bf16)
            spread = lax.all_to_all(
                summed.reshape(np_, own_rows, part), ("y", "x"), 0, 0, tiled=True
            )
            return jnp.transpose(spread.astype(f32), (1, 0, 2)).reshape(own_rows, hidden)

        shrink_gradient = hidden_gradient(
            jnp.concatenate(cot_blocks, axis=0), jnp.concatenate(act_blocks, axis=0)
        )
        expand_gradient = hidden_gradient(
            jnp.concatenate(mid_blocks, axis=0), jnp.concatenate(slope_blocks, axis=0)
        )

        def by_c(values):
            rows = values.shape[0]
            return jnp.transpose(
                values.reshape(rows, ny, nc, n1 * n2 * own_rows), (0, 2, 1, 3)
            ).reshape(rows, nc, width // nc)

        def plane_sum(rows):
            columns_ = rows.shape[-1]
            rows = rows.reshape(ny, n1, n2, own_rows, columns_)

            def towards(dy, dx):
                block = lax.dynamic_index_in_dim(rows, (yi + dy) % ny, 0, keepdims=False)
                return lax.dynamic_index_in_dim(block, (xi + dx) % n2, 1, keepdims=False)

            result = towards(0, 0)
            for dy, dx in plane[1:]:
                result = result + shift_plane(towards(dy, dx).astype(bf16), dy, dx).astype(f32)
            return result

        mixing_rows = plane_sum(chip_pair(by_c(attended), branch_slope, False))
        mixing_gradient = jnp.sum(
            lax.all_to_all(mixing_rows.astype(bf16), "z", 0, 0, tiled=True).astype(f32), axis=0
        )
        joint_rows = plane_sum(chip_pair(by_c(line_normed), joint_slope, False))
        joint_spread = lax.all_to_all(joint_rows.astype(bf16), "z", 0, 0, tiled=True)
        joint_gradient = jnp.transpose(joint_spread.astype(f32), (1, 0, 2)).reshape(
            own_rows, 3 * width
        )

        def column_sum(values):
            return jnp.sum(values.astype(f32), axis=0)

        hidden_sums = functools.reduce(jnp.add, [column_sum(s) for s in slope_blocks])
        early = lax.psum(
            jnp.concatenate(
                [
                    column_sum(branch_slope),
                    column_sum(normed_slope * normal2),
                    column_sum(normed_slope),
                    column_sum(cotangent),
                    lax.dynamic_update_slice(
                        jnp.zeros((hidden,), f32), hidden_sums, (plane_index * part,)
                    ),
                ]
            ),
            ALL,
        )
        empty = jnp.zeros((width,), f32)
        first_column = (zi * n2 + xi) * span
        late = jnp.sum(
            lax.all_gather(
                jnp.concatenate(
                    [
                        column_sum(entry_slope * normal1),
                        column_sum(entry_slope),
                        lax.dynamic_update_slice(
                            empty, own_sums[:, 0].reshape(span), (first_column,)
                        ),
                        lax.dynamic_update_slice(
                            empty, own_sums[:, 2].reshape(span), (first_column,)
                        ),
                    ]
                ),
                ALL,
                axis=0,
                tiled=False,
            ),
            axis=0,
        )
        return (
            layer_output,
            input_gradient,
            late[:width],
            late[width : 2 * width],
            joint_gradient,
            late[2 * width : 3 * width],
            late[3 * width :],
            mixing_gradient,
            early[:width],
            early[width : 2 * width],
            early[2 * width : 3 * width],
            expand_gradient,
            early[4 * width :],
            shrink_gradient,
            early[3 * width : 4 * width],
        )

    rows = P(ALL, None)
    group = P(("y", "c"), None)
    return jax.shard_map(
        shards,
        mesh=fine,
        in_specs=(
            rows,
            P(),
            P(),
            rows,
            P(),
            P(),
            rows,
            P(),
            P(),
            P(),
            rows,
            P(),
            rows,
            P(),
            group,
            group,
            rows,
        ),
        out_specs=(
            rows,
            rows,
            P(),
            P(),
            rows,
            P(),
            P(),
            rows,
            P(),
            P(),
            P(),
            rows,
            P(),
            rows,
            P(),
        ),
        check_vma=False,
    )
```
